32 devices in a mesh: tp: 4 (over z), cp: 2 (over x), dp: 4 (over y, core).
Axes of the slice: x: 2, y: 2, z: 4, core: 2. Of those that a mesh axis runs over, the one named last changes fastest.
Arguments:
- tokens: bfloat16 [2048, 7168], P(('dp', 'tp', 'cp')), parts along dimension 0, may hold values from -6 to 6
- router: bfloat16 [7168, 4], replicated, may hold values from -0.0625 to 0.0625
- gate_weight: bfloat16 [4, 7168, 1024], P('cp', None, 'tp'), may hold values from -0.0625 to 0.0625
- up_weight: bfloat16 [4, 7168, 1024], P('cp', None, 'tp'), may hold values from -0.0625 to 0.0625
- down_weight: bfloat16 [4, 1024, 7168], P('cp', 'tp'), may hold values from -0.1875 to 0.1875
- expert_ids: int32 [2048, 2], P(('dp', 'tp', 'cp')), parts along dimension 0, may hold values from 0 to 3, as said below
- slot_index: int32 [2048, 2], P(('dp', 'tp', 'cp')), parts along dimension 0, may hold values from -1 to 1, as said below
Outputs:
- moe_out: bfloat16 [2048, 7168], P(('dp', 'tp', 'cp')), parts along dimension 0
The draws below stay inside these ranges and needn't reach their ends.
There are 4 independent parts, one for each index of `dp`. The reference program is written for one: setup_inputs(seed, part) draws one part's arguments, and reference() takes and returns one part's arrays. A program takes and returns all parts, laid end to end along the dimension named above; an argument that names none is the same for every part. Nothing has to cross between parts.
Inputs may be any that keep to these rules, and one draw needn't show every extreme that they name: `expert_ids`: each row names 2 different experts in rising order; in every part one expert is named by 32 or more rows of every block. slot_index[t, k] is the number of earlier copies to expert expert_ids[t, k] within token t's block (rows in order, then k in order) when that is below 2, else -1.
All inputs are finite; a program needn't handle non-finite values.
Results may differ from the reference program's by a relative error of at most 0.012.
Values may be sent and summed in bfloat16 or wider, within the bound.
A program may use at most 64 MiB of HBM per device.

```python
import jax
import jax.numpy as jnp
from jax import lax

D = 7168
FF = 1024
TOP = 2
TOK_DEV = 64
CAP_DEV = 2
SPECIALIST_COUNT = 4
FF_DEV = 256
TOKENS = 512
N_TP = 4
N_CP = 2


def routing(key):
    blocks = N_TP * N_CP
    key_hot, key_noise, key_bias, key_rank = jax.random.split(key, 4)
    crowded_specialist = jax.random.randint(key_hot, (), 0, SPECIALIST_COUNT)
    normal_perturbation = jax.random.randint(key_noise, (blocks, TOK_DEV, SPECIALIST_COUNT), 0, 1 << 16)
    dispatcher_offset = jax.random.randint(key_bias, (blocks, 1, SPECIALIST_COUNT), 0, 1 << 15)
    order = jax.random.randint(key_rank, (blocks, TOK_DEV), 0, 1 << 20) * TOK_DEV + jnp.arange(TOK_DEV, dtype=jnp.int32)[None, :]
    ranking = jnp.argsort(jnp.argsort(order, axis=1, stable=True), axis=1, stable=True)
    preferred_specialist = ranking < TOK_DEV // 2
    uniform_samples = jnp.arange(SPECIALIST_COUNT, dtype=jnp.int32)
    preference_offset = jnp.where(preferred_specialist[:, :, None] & (uniform_samples[None, None, :] == crowded_specialist), 1 << 17, 0)
    dispatcher_logit = (normal_perturbation + dispatcher_offset + preference_offset) * SPECIALIST_COUNT + uniform_samples[None, None, :]
    top_values, top_ids = lax.top_k(dispatcher_logit, TOP)
    chosen_ids = jnp.sort(top_ids.astype(jnp.int32), axis=-1)
    onehot = (chosen_ids[:, :, :, None] == uniform_samples).astype(jnp.int32).reshape(blocks, TOK_DEV * TOP, SPECIALIST_COUNT)
    earlier = jnp.cumsum(onehot, axis=1) - onehot
    position = jnp.sum(earlier * onehot, axis=-1).reshape(blocks, TOK_DEV, TOP)
    slot_values = jnp.where(position < CAP_DEV, position, -1).astype(jnp.int32)
    return (chosen_ids.reshape(TOKENS, TOP), slot_values.reshape(TOKENS, TOP))


def draw_expert_ids(key, part):
    return routing(jax.random.fold_in(key, 11))[0]


def draw_slot_index(key, part):
    return routing(jax.random.fold_in(key, 11))[1]


def level_of(key, shape, cuts, least, largest):
    def one(axis_at, parts):
        draws = jax.random.uniform(jax.random.fold_in(jax.random.fold_in(key, 6), axis_at), (parts,), jnp.float32, least / len(cuts), largest / len(cuts))
        return jnp.repeat(jnp.exp(draws), shape[axis_at] // parts).reshape((-1,) + (1,) * (len(shape) - axis_at - 1))

    level = one(*cuts[0])
    for cut in cuts[1:]:
        level = level * one(*cut)
    return level


def gaussian(own_key, shape, width, limit, shards=(), kind=jnp.bfloat16):
    drawn = jax.random.normal(own_key, shape, jnp.float32) * width
    if len(shards) > 0:
        drawn = level_of(own_key, shape, shards, -0.22, 0.18) * drawn
    return jnp.clip(drawn, min=-limit, max=limit).astype(kind)


def setup_inputs(seed: int = 0, part: int = 0) -> dict:
    arg_keys = jax.random.split(jax.random.key(seed), 8)
    part_splits = jax.random.split(jax.random.fold_in(arg_keys[7], part), 8)
    return {
        "tokens": gaussian(part_splits[0], (TOKENS, D), 1.0, 6.0, ((0, 8),)),
        "router": gaussian(arg_keys[1], (D, SPECIALIST_COUNT), D ** -0.5, 0.0625),
        "gate_weight": gaussian(arg_keys[2], (SPECIALIST_COUNT, D, FF), D ** -0.5, 0.0625, ((0, 2), (2, 4))),
        "up_weight": gaussian(arg_keys[3], (SPECIALIST_COUNT, D, FF), D ** -0.5, 0.0625, ((0, 2), (2, 4))),
        "down_weight": gaussian(arg_keys[4], (SPECIALIST_COUNT, FF, D), FF ** -0.5, 0.1875, ((0, 2), (1, 4))),
        "expert_ids": draw_expert_ids(jax.random.fold_in(jax.random.fold_in(arg_keys[7], part), 71), part),
        "slot_index": draw_slot_index(jax.random.fold_in(jax.random.fold_in(arg_keys[7], part), 71), part),
    }


route_scale = 2.5


def reference(tokens, router, gate_weight, up_weight, down_weight, expert_ids, slot_index):
    logits = jnp.dot(tokens, router, preferred_element_type=jnp.float32)
    affinity = jax.nn.sigmoid(logits)
    chosen = jnp.take_along_axis(affinity, expert_ids, axis=1)
    gate_share = route_scale * chosen / jnp.sum(chosen, axis=1, keepdims=True)
    blocks = N_TP * N_CP
    token_block = (jnp.arange(TOKENS) // TOK_DEV).astype(jnp.int32)
    slot_total = SPECIALIST_COUNT * blocks * CAP_DEV
    destination = jnp.where(slot_index >= 0, expert_ids * (blocks * CAP_DEV) + token_block[:, None] * CAP_DEV + slot_index, slot_total).astype(jnp.int32)
    buffer = jnp.zeros((slot_total + 1, D), jnp.bfloat16)
    buffer = buffer.at[destination.reshape(-1)].set(jnp.repeat(tokens, TOP, axis=0))
    dispatched = buffer[:slot_total].reshape(SPECIALIST_COUNT, blocks * CAP_DEV, D)

    def one_expert(pieces):
        expert_rows, w_gate, w_up, w_down = pieces
        gate_part = jnp.dot(expert_rows, w_gate, preferred_element_type=jnp.float32)
        up_part = jnp.dot(expert_rows, w_up, preferred_element_type=jnp.float32)
        hidden = (jax.nn.silu(gate_part) * up_part).astype(jnp.bfloat16)
        grouped = hidden.reshape(blocks * CAP_DEV, N_TP, FF_DEV).astype(jnp.float32)
        down_groups = w_down.reshape(N_TP, FF_DEV, D).astype(jnp.float32)
        partial_value = jnp.einsum("mgf,gfd->gmd", grouped, down_groups).astype(jnp.bfloat16)
        partial_value = lax.optimization_barrier(partial_value)
        return jnp.sum(partial_value.astype(jnp.float32), axis=0)

    expert_out = lax.map(one_expert, (dispatched, gate_weight, up_weight, down_weight))
    flat_index = (expert_ids * (blocks * CAP_DEV) + token_block[:, None] * CAP_DEV + jnp.maximum(slot_index, 0)).astype(jnp.int32)
    picked = expert_out.reshape(slot_total, D)[flat_index]
    weight = jnp.where(slot_index >= 0, gate_share, jnp.float32(0.0))
    return jnp.sum(picked * weight[:, :, None], axis=1).astype(jnp.bfloat16)
```

```python
import functools

import jax
import jax.numpy as jnp
from jax import lax
from jax.experimental import pallas as pl
from jax.experimental.pallas import tpu as pltpu
from jax.sharding import PartitionSpec as P

CAP_DEV = 2
ROUTE_SCALE = 2.5
MESH = pl.DeviceIdType.MESH
NT = (((1,), (1,)), ((), ()))
TN = (((0,), (0,)), ((), ()))


def rows_of(ref, c):
    pieces = [ref[c, i].astype(jnp.float32) for i in range(ref.shape[1])]
    return jnp.concatenate(pieces, axis=0).astype(jnp.bfloat16)


def kernel(
    n_tp, n_cp, nc,
    tok_hbm, rt_hbm, ids_ref, slot_ref, wg_hbm, wu_hbm, wd_hbm,
    out_hbm,
    tok, rt, wg, wu, wd, xs, xr, ps, pr, ob,
    in_sem, wsem, osem, s1, r1, s2, r2,
):
    n = n_tp * n_cp
    my_z, my_x = lax.axis_index("tp"), lax.axis_index("cp")
    me = my_z * n_cp + my_x
    local, width, ff = wg.shape
    rpp = xr.shape[2]
    dc = width // nc
    slots = n_cp * rpp

    tok_copy = pltpu.make_async_copy(tok_hbm, tok, in_sem.at[0])
    tok_copy.start()
    rt_copy = pltpu.make_async_copy(rt_hbm, rt, in_sem.at[1])
    rt_copy.start()

    def peer(j):
        other = lax.rem(me + j, n)
        return other, {"tp": other // n_cp, "cp": lax.rem(other, n_cp)}

    barrier = pltpu.get_barrier_semaphore()
    for j in range(1, n):
        pl.semaphore_signal(barrier, inc=1, device_id=peer(j)[1], device_id_type=MESH)

    up_copies, down_copies = [], []
    for c in range(nc):
        cols = pl.ds(c * dc, dc)
        pair = [
            pltpu.make_async_copy(wg_hbm.at[:, cols, :], wg.at[:, cols, :], wsem.at[0, c]),
            pltpu.make_async_copy(wu_hbm.at[:, cols, :], wu.at[:, cols, :], wsem.at[1, c]),
        ]
        for copy in pair:
            copy.start()
        up_copies.append(pair)
    for c in range(nc):
        cols = pl.ds(c * dc, dc)
        copy = pltpu.make_async_copy(wd_hbm.at[:, :, cols], wd.at[:, :, cols], wsem.at[2, c])
        copy.start()
        down_copies.append(copy)

    ids0, ids1 = ids_ref[0:1, :], ids_ref[1:2, :]
    slot0, slot1 = slot_ref[0:1, :], slot_ref[1:2, :]
    target0 = jnp.where(slot0 >= 0, ids0 * CAP_DEV + slot0, -1)
    target1 = jnp.where(slot1 >= 0, ids1 * CAP_DEV + slot1, -1)
    row = lax.broadcasted_iota(jnp.int32, (slots, ids0.shape[1]), 0)
    placing = jnp.where((row == target0) | (row == target1), 1.0, 0.0).astype(jnp.bfloat16)

    tok_copy.wait()
    first = []
    for c in range(nc):
        cols = pl.ds(c * dc, dc)
        outgoing = jnp.dot(placing, tok[:, cols], preferred_element_type=jnp.float32)
        for x in range(n_cp):
            xs[c, x] = outgoing[x * rpp:(x + 1) * rpp].astype(jnp.bfloat16)
        if c == 0:
            pl.semaphore_wait(barrier, n - 1)
        for j in range(1, n):
            other, where = peer(j)
            copy = pltpu.make_async_remote_copy(
                src_ref=xs.at[c, lax.rem(other, n_cp)],
                dst_ref=xr.at[c, me],
                send_sem=s1.at[c, j],
                recv_sem=r1.at[c, j],
                device_id=where,
                device_id_type=MESH,
            )
            copy.start()
            first.append(copy)
        xr[c, me] = xs[c, my_x]

    rt_copy.wait()
    logits = lax.dot_general(rt[...], tok[...], NT, preferred_element_type=jnp.float32)
    affinity = 1.0 / (1.0 + jnp.exp(-logits))
    erow = lax.broadcasted_iota(jnp.int32, logits.shape, 0)
    chosen0 = jnp.sum(jnp.where(erow == ids0, affinity, 0.0), axis=0, keepdims=True)
    chosen1 = jnp.sum(jnp.where(erow == ids1, affinity, 0.0), axis=0, keepdims=True)
    total = chosen0 + chosen1
    share0 = ROUTE_SCALE * chosen0 / total
    share1 = ROUTE_SCALE * chosen1 / total
    wide = lax.rem(lax.broadcasted_iota(jnp.int32, (n * rpp, ids0.shape[1]), 0), slots)
    mix = jnp.where(wide == target0, share0, 0.0) + jnp.where(wide == target1, share1, 0.0)
    mix = mix.T
    mix_hi = mix.astype(jnp.bfloat16)
    mix_lo = (mix - mix_hi.astype(jnp.float32)).astype(jnp.bfloat16)
    mix_both = jnp.concatenate([mix_hi, mix_lo], axis=0)

    def arrival(buf, c, j, sem):
        source = lax.rem(me + n - j, n)
        ref = buf.at[c, source]
        pltpu.make_async_remote_copy(
            src_ref=ref, dst_ref=ref, send_sem=sem.at[c, j], recv_sem=sem.at[c, j],
            device_id=peer(n - j)[1], device_id_type=MESH,
        ).wait_recv()

    gate = [jnp.zeros((n * rpp, ff), jnp.float32) for _ in range(local)]
    up = [jnp.zeros((n * rpp, ff), jnp.float32) for _ in range(local)]
    for c in range(nc):
        cols = pl.ds(c * dc, dc)
        for copy in up_copies[c]:
            copy.wait()
        for j in range(1, n):
            arrival(xr, c, j, r1)
        x = rows_of(xr, c)
        for e in range(local):
            gate[e] += jnp.dot(x, wg[e, cols, :], preferred_element_type=jnp.float32)
            up[e] += jnp.dot(x, wu[e, cols, :], preferred_element_type=jnp.float32)
    owner = lax.rem(lax.broadcasted_iota(jnp.int32, (n * rpp, ff), 0), rpp) // CAP_DEV
    hidden = []
    for e in range(local):
        value = gate[e] / (1.0 + jnp.exp(-gate[e])) * up[e]
        hidden.append(jnp.where(owner == e, value, 0.0).astype(jnp.bfloat16))

    second = []
    for c in range(nc):
        cols = pl.ds(c * dc, dc)
        down_copies[c].wait()
        part = jnp.dot(hidden[0], wd[0, :, cols], preferred_element_type=jnp.float32)
        for e in range(1, local):
            part += jnp.dot(hidden[e], wd[e, :, cols], preferred_element_type=jnp.float32)
        for i in range(n):
            ps[c, i] = part[i * rpp:(i + 1) * rpp].astype(jnp.bfloat16)
        for j in range(1, n):
            other, where = peer(j)
            copy = pltpu.make_async_remote_copy(
                src_ref=ps.at[c, other],
                dst_ref=pr.at[c, me],
                send_sem=s2.at[c, j],
                recv_sem=r2.at[c, j],
                device_id=where,
                device_id_type=MESH,
            )
            copy.start()
            second.append(copy)
        pr[c, me] = ps[c, me]

    half = mix.shape[0]
    outs = []
    for c in range(nc):
        cols = pl.ds(c * dc, dc)
        for j in range(1, n):
            arrival(pr, c, j, r2)
        both = jnp.dot(mix_both, rows_of(pr, c), preferred_element_type=jnp.float32)
        ob[:, cols] = (both[:half] + both[half:]).astype(jnp.bfloat16)
        copy = pltpu.make_async_copy(ob.at[:, cols], out_hbm.at[:, cols], osem.at[c])
        copy.start()
        outs.append(copy)
    for copy in first + second:
        copy.wait_send()
    for copy in outs:
        copy.wait()


def body(n_tp, n_cp, tokens, router, gate_weight, up_weight, down_weight, expert_ids, slot_index):
    n = n_tp * n_cp
    rows, width = tokens.shape
    local, _, ff = gate_weight.shape
    rpp = local * CAP_DEV
    nc = 4 if n <= 16 else 1
    dc = width // nc
    anywhere = pl.BlockSpec(memory_space=pl.ANY)
    vmem = pl.BlockSpec(memory_space=pltpu.VMEM)
    bf16 = jnp.bfloat16
    dma = pltpu.SemaphoreType.DMA
    return pl.pallas_call(
        functools.partial(kernel, n_tp, n_cp, nc),
        out_shape=jax.ShapeDtypeStruct((rows, width), bf16),
        in_specs=[anywhere, anywhere, vmem, vmem, anywhere, anywhere, anywhere],
        out_specs=anywhere,
        scratch_shapes=[
            pltpu.VMEM((rows, width), bf16),
            pltpu.VMEM((router.shape[1], width), bf16),
            pltpu.VMEM((local, width, ff), bf16),
            pltpu.VMEM((local, width, ff), bf16),
            pltpu.VMEM((local, ff, width), bf16),
            pltpu.VMEM((nc, n_cp, rpp, dc), bf16),
            pltpu.VMEM((nc, n, rpp, dc), bf16),
            pltpu.VMEM((nc, n, rpp, dc), bf16),
            pltpu.VMEM((nc, n, rpp, dc), bf16),
            pltpu.VMEM((rows, width), bf16),
            dma((2,)),
            dma((3, nc)),
            dma((nc,)),
            dma((nc, n)),
            dma((nc, n)),
            dma((nc, n)),
            dma((nc, n)),
        ],
        compiler_params=pltpu.CompilerParams(
            collective_id=0, has_side_effects=True, vmem_limit_bytes=60 * 1024 * 1024
        ),
    )(tokens, router.T, expert_ids.T, slot_index.T, gate_weight, up_weight, down_weight)


def solution(mesh):
    in_specs = (
        P(("dp", "tp", "cp"), None),
        P(),
        P("cp", None, "tp"),
        P("cp", None, "tp"),
        P("cp", "tp", None),
        P(("dp", "tp", "cp"), None),
        P(("dp", "tp", "cp"), None),
    )
    out_specs = P(("dp", "tp", "cp"), None)
    step = functools.partial(body, mesh.shape["tp"], mesh.shape["cp"])
    return jax.shard_map(step, mesh=mesh, in_specs=in_specs, out_specs=out_specs, check_vma=False)
```

```python
import functools

import jax
import jax.numpy as jnp
from jax import lax
from jax.experimental import pallas as pl
from jax.experimental.pallas import tpu as pltpu
from jax.sharding import PartitionSpec as P

CAP_DEV = 2
ROUTE_SCALE = 2.5
CHUNKS = 1
MESH = pl.DeviceIdType.MESH
NT = (((1,), (1,)), ((), ()))


def rows_of(pieces):
    return jnp.concatenate([p.astype(jnp.float32) for p in pieces], axis=0).astype(jnp.bfloat16)


def flip(index, bits):
    for b in range(bits.bit_length()):
        if (bits >> b) & 1:
            index = index + (1 - 2 * lax.rem(index // (1 << b), 2)) * (1 << b)
    return index


def exchange_kernel(
    n_tp, n_cp, nc,
    tok_hbm, rt_hbm, ids_hbm, slot_hbm, wg_hbm, wu_hbm, wd_hbm,
    pr, mix_hbm,
    ids_ref, slot_ref, tok, rt, wg, wu, wd, xs, xr, ps, mix_ref,
    in_sem, wsem, own_sem, s1, r1, s2, r2,
):
    n = n_tp * n_cp
    my_z, my_x = lax.axis_index("tp"), lax.axis_index("cp")
    me = my_z * n_cp + my_x
    local, width, ff = wg.shape
    dc = width // nc
    slots = n_cp * local * CAP_DEV
    pow2 = n & (n - 1) == 0
    order = list(range(n - 1, 0, -1))

    def peer(j):
        return flip(me, j) if pow2 else lax.rem(me + j, n)

    def source(j):
        return flip(me, j) if pow2 else lax.rem(me + n - j, n)

    def device(other):
        return {"tp": other // n_cp, "cp": lax.rem(other, n_cp)}

    index_copies = [
        pltpu.make_async_copy(ids_hbm, ids_ref, in_sem.at[nc + 2]),
        pltpu.make_async_copy(slot_hbm, slot_ref, in_sem.at[nc + 3]),
    ]
    for copy in index_copies:
        copy.start()
    tok_copies = []
    for c in range(nc):
        cols = pl.ds(c * dc, dc)
        copy = pltpu.make_async_copy(tok_hbm.at[:, cols], tok.at[:, cols], in_sem.at[c])
        copy.start()
        tok_copies.append(copy)
    rt_copy = pltpu.make_async_copy(rt_hbm, rt, in_sem.at[nc])
    rt_copy.start()

    barrier = pltpu.get_barrier_semaphore()
    for j in order:
        pl.semaphore_signal(barrier, inc=1, device_id=device(peer(j)), device_id_type=MESH)

    up_copies, down_copies = {}, {}
    for e in range(local):
        for c in range(nc):
            cols = pl.ds(c * dc, dc)
            pair = [
                pltpu.make_async_copy(wg_hbm.at[e, cols, :], wg.at[e, cols, :], wsem.at[0, e, c]),
                pltpu.make_async_copy(wu_hbm.at[e, cols, :], wu.at[e, cols, :], wsem.at[1, e, c]),
            ]
            for copy in pair:
                copy.start()
            up_copies[e, c] = pair
        for c in range(nc):
            cols = pl.ds(c * dc, dc)
            copy = pltpu.make_async_copy(wd_hbm.at[e, :, cols], wd.at[e, :, cols], wsem.at[2, e, c])
            copy.start()
            down_copies[e, c] = copy

    for copy in index_copies:
        copy.wait()
    ids0, ids1 = ids_ref[0:1, :], ids_ref[1:2, :]
    slot0, slot1 = slot_ref[0:1, :], slot_ref[1:2, :]
    target0 = jnp.where(slot0 >= 0, ids0 * CAP_DEV + slot0, -1)
    target1 = jnp.where(slot1 >= 0, ids1 * CAP_DEV + slot1, -1)
    row = lax.broadcasted_iota(jnp.int32, (slots, ids0.shape[1]), 0)
    placing = jnp.where((row == target0) | (row == target1), 1.0, 0.0).astype(jnp.bfloat16)

    sends = []

    def dispatch(e, c):
        for j in order:
            other = peer(j)
            copy = pltpu.make_async_remote_copy(
                src_ref=xs.at[e, c, lax.rem(other, n_cp)],
                dst_ref=xr.at[e, c, me],
                send_sem=s1.at[e, c, j],
                recv_sem=r1.at[e, c, j],
                device_id=device(other),
                device_id_type=MESH,
            )
            copy.start()
            sends.append(copy)
        xr[e, c, me] = xs[e, c, my_x]

    for c in range(nc):
        tok_copies[c].wait()
        cols = pl.ds(c * dc, dc)
        outgoing = jnp.dot(placing, tok[:, cols], preferred_element_type=jnp.float32)
        for x in range(n_cp):
            for e in range(local):
                at = (x * local + e) * CAP_DEV
                xs[e, c, x] = outgoing[at:at + CAP_DEV].astype(jnp.bfloat16)
        if c == 0:
            pl.semaphore_wait(barrier, n - 1)
        dispatch(0, c)
    for e in range(1, local):
        for c in range(nc):
            dispatch(e, c)

    rt_copy.wait()
    logits = lax.dot_general(rt[...], tok[...], NT, preferred_element_type=jnp.float32)
    affinity = 1.0 / (1.0 + jnp.exp(-logits))
    erow = lax.broadcasted_iota(jnp.int32, logits.shape, 0)
    chosen0 = jnp.sum(jnp.where(erow == ids0, affinity, 0.0), axis=0, keepdims=True)
    chosen1 = jnp.sum(jnp.where(erow == ids1, affinity, 0.0), axis=0, keepdims=True)
    total = chosen0 + chosen1
    share0 = ROUTE_SCALE * chosen0 / total
    share1 = ROUTE_SCALE * chosen1 / total
    wide = lax.broadcasted_iota(jnp.int32, (local * n * CAP_DEV, ids0.shape[1]), 0)
    which = lax.rem(wide // CAP_DEV, n_cp) * local + wide // (n * CAP_DEV)
    wide = which * CAP_DEV + lax.rem(wide, CAP_DEV)
    mix = jnp.where(wide == target0, share0, 0.0) + jnp.where(wide == target1, share1, 0.0)
    mix = mix.T
    mix_hi = mix.astype(jnp.bfloat16)
    mix_lo = (mix - mix_hi.astype(jnp.float32)).astype(jnp.bfloat16)
    mix_ref[...] = jnp.concatenate([mix_hi, mix_lo], axis=0)
    mix_copy = pltpu.make_async_copy(mix_ref, mix_hbm, in_sem.at[nc + 1])
    mix_copy.start()

    def arrival(ref, j, sem):
        pltpu.make_async_remote_copy(
            src_ref=ref, dst_ref=ref, send_sem=sem, recv_sem=sem,
            device_id=device(peer(j)), device_id_type=MESH,
        ).wait_recv()

    owns = []
    for e in range(local):
        gate = jnp.zeros((n * CAP_DEV, ff), jnp.float32)
        up = jnp.zeros((n * CAP_DEV, ff), jnp.float32)
        for c in range(nc):
            cols = pl.ds(c * dc, dc)
            for copy in up_copies[e, c]:
                copy.wait()
            for j in order:
                arrival(xr.at[e, c, source(j)], j, r1.at[e, c, j])
            x = rows_of([xr[e, c, i] for i in range(n)])
            gate += jnp.dot(x, wg[e, cols, :], preferred_element_type=jnp.float32)
            up += jnp.dot(x, wu[e, cols, :], preferred_element_type=jnp.float32)
        hidden = (gate / (1.0 + jnp.exp(-gate)) * up).astype(jnp.bfloat16)
        for c in range(nc):
            cols = pl.ds(c * dc, dc)
            down_copies[e, c].wait()
            part = jnp.dot(hidden, wd[e, :, cols], preferred_element_type=jnp.float32)
            for i in range(n):
                ps[e, c, i] = part[i * CAP_DEV:(i + 1) * CAP_DEV].astype(jnp.bfloat16)
            for j in order:
                other = peer(j)
                copy = pltpu.make_async_remote_copy(
                    src_ref=ps.at[e, c, other],
                    dst_ref=pr.at[e, c, me],
                    send_sem=s2.at[e, c, j],
                    recv_sem=r2.at[e, c, j],
                    device_id=device(other),
                    device_id_type=MESH,
                )
                copy.start()
                sends.append(copy)
            own = pltpu.make_async_copy(ps.at[e, c, me], pr.at[e, c, me], own_sem.at[e, c])
            own.start()
            owns.append(own)
    mix_copy.wait()
    for copy in owns:
        copy.wait()
    for copy in sends:
        copy.wait_send()
    for e in range(local):
        for c in range(nc):
            for j in order:
                arrival(pr.at[e, c, source(j)], j, r2.at[e, c, j])


def combine_kernel(pr_hbm, mix_hbm, out_hbm, pr, mix_ref, ob, isem, osem):
    local, nc, n, cap, dc = pr.shape
    mix_copy = pltpu.make_async_copy(mix_hbm, mix_ref, isem.at[nc])
    mix_copy.start()
    loads, outs = [], []
    for c in range(nc):
        copy = pltpu.make_async_copy(pr_hbm.at[:, c], pr.at[:, c], isem.at[c])
        copy.start()
        loads.append(copy)
    mix_copy.wait()
    mix = mix_ref[...]
    half = mix.shape[0] // 2
    for c in range(nc):
        loads[c].wait()
        rows = rows_of([pr[e, c, i] for e in range(local) for i in range(n)])
        for p in range(2):
            part = dc // 2
            cols = pl.ds(c * dc + p * part, part)
            both = jnp.dot(
                mix, rows[:, p * part:(p + 1) * part], preferred_element_type=jnp.float32
            )
            ob[:, cols] = (both[:half] + both[half:]).astype(jnp.bfloat16)
            copy = pltpu.make_async_copy(ob.at[:, cols], out_hbm.at[:, cols], osem.at[c, p])
            copy.start()
            outs.append(copy)
    for copy in outs:
        copy.wait()


def body(n_tp, n_cp, tokens, router, gate_weight, up_weight, down_weight, expert_ids, slot_index):
    n = n_tp * n_cp
    rows, width = tokens.shape
    local, _, ff = gate_weight.shape
    nc = CHUNKS if n <= 16 else 1
    dc = width // nc
    anywhere = pl.BlockSpec(memory_space=pl.ANY)
    bf16 = jnp.bfloat16
    dma = pltpu.SemaphoreType.DMA
    slab = (local, nc, n, CAP_DEV, dc)
    pr, mix = pl.pallas_call(
        functools.partial(exchange_kernel, n_tp, n_cp, nc),
        out_shape=[
            jax.ShapeDtypeStruct(slab, bf16),
            jax.ShapeDtypeStruct((2 * rows, local * n * CAP_DEV), bf16),
        ],
        in_specs=[anywhere] * 7,
        out_specs=[anywhere, anywhere],
        scratch_shapes=[
            pltpu.VMEM((expert_ids.shape[1], rows), jnp.int32),
            pltpu.VMEM((slot_index.shape[1], rows), jnp.int32),
            pltpu.VMEM((rows, width), bf16),
            pltpu.VMEM((router.shape[1], width), bf16),
            pltpu.VMEM((local, width, ff), bf16),
            pltpu.VMEM((local, width, ff), bf16),
            pltpu.VMEM((local, ff, width), bf16),
            pltpu.VMEM((local, nc, n_cp, CAP_DEV, dc), bf16),
            pltpu.VMEM(slab, bf16),
            pltpu.VMEM(slab, bf16),
            pltpu.VMEM((2 * rows, local * n * CAP_DEV), bf16),
            dma((nc + 4,)),
            dma((3, local, nc)),
            dma((local, nc)),
            dma((local, nc, n)),
            dma((local, nc, n)),
            dma((local, nc, n)),
            dma((local, nc, n)),
        ],
        compiler_params=pltpu.CompilerParams(
            collective_id=0, has_side_effects=True, vmem_limit_bytes=60 * 1024 * 1024
        ),
    )(tokens, router.T, expert_ids.T, slot_index.T, gate_weight, up_weight, down_weight)
    return pl.pallas_call(
        combine_kernel,
        out_shape=jax.ShapeDtypeStruct((rows, width), bf16),
        in_specs=[anywhere, anywhere],
        out_specs=anywhere,
        scratch_shapes=[
            pltpu.VMEM(slab, bf16),
            pltpu.VMEM(mix.shape, bf16),
            pltpu.VMEM((rows, width), bf16),
            dma((nc + 1,)),
            dma((nc, 2)),
        ],
    )(pr, mix)


def solution(mesh):
    in_specs = (
        P(("dp", "tp", "cp"), None),
        P(),
        P("cp", None, "tp"),
        P("cp", None, "tp"),
        P("cp", "tp", None),
        P(("dp", "tp", "cp"), None),
        P(("dp", "tp", "cp"), None),
    )
    out_specs = P(("dp", "tp", "cp"), None)
    step = functools.partial(body, mesh.shape["tp"], mesh.shape["cp"])
    return jax.shard_map(step, mesh=mesh, in_specs=in_specs, out_specs=out_specs, check_vma=False)
```
